32 devices in a mesh: row: 8 (over y, x, core), col: 4 (over z).
Axes of the slice: x: 2, y: 2, z: 4, core: 2. Of those that a mesh axis runs over, the one named last changes fastest.
Arguments:
- source: float32 [512, 512, 512], P('row', 'col'), may hold values from -8 to 8
- basis_x: float32 [512, 512], replicated, may hold values from -0.25 to 0.25
- basis_y: float32 [512, 512], replicated, may hold values from -0.25 to 0.25
- basis_z: float32 [512, 512], replicated, may hold values from -0.25 to 0.25
- eigen_x: float32 [512], replicated, may hold values from 0.1 to 10
- eigen_y: float32 [512], replicated, may hold values from 0.1 to 10
- eigen_z: float32 [512], replicated, may hold values from 0.1 to 10
Outputs:
- solution: float32 [512, 512, 512], P('row', 'col')
The draws below stay inside these ranges and needn't reach their ends.
All inputs are finite; a program needn't handle non-finite values.
Results may differ from the reference program's by a relative error of at most 0.00007.
Values sent between devices are 32-bit elements; how exact they have to be, the bound alone decides.
A program may use at most 128 MiB of HBM per device.

```python
import math
import jax
import jax.numpy as jnp
from jax import lax

NX = 512
NY = 512
NZ = 512


def levels(stream_key, extent, cuts, smallest, top_value):
    level, own = 1.0, jax.random.fold_in(stream_key, 6)
    for axis_at, parts in cuts:
        draws = jnp.exp(jax.random.uniform(jax.random.fold_in(own, axis_at), (parts,), jnp.float32, smallest / len(cuts), top_value / len(cuts)))
        level = level * jnp.repeat(draws, extent[axis_at] // parts).reshape([-1 if axis == axis_at else 1 for axis in range(len(extent))])
    return level


def gaussian(stream_key, extent, width, limit, split=(), held_as=jnp.bfloat16):
    values = jax.random.normal(stream_key, extent, jnp.float32) * width
    if len(split) > 0:
        values = levels(stream_key, extent, split, -0.22, 0.18) * values
    return jnp.clip(values, min=-limit, max=limit).astype(held_as)


def setup_inputs(seed: int = 0) -> dict:
    keys = jax.random.split(jax.random.key(seed), 8)
    source = gaussian(keys[0], (NX, NY, NZ), 1.0, 8.0, ((0, 8), (1, 4)), jnp.float32)
    basis_x = gaussian(keys[1], (NX, NX), NX ** -0.5, 0.25, (), jnp.float32)
    basis_y = gaussian(keys[2], (NY, NY), NY ** -0.5, 0.25, (), jnp.float32)
    basis_z = gaussian(keys[3], (NZ, NZ), NZ ** -0.5, 0.25, (), jnp.float32)
    eigen_x = jnp.clip(jnp.exp(jax.random.uniform(keys[4], (NX,), jnp.float32, math.log(0.1), math.log(10.0))), 0.1, 10.0)
    eigen_y = jnp.clip(jnp.exp(jax.random.uniform(keys[5], (NY,), jnp.float32, math.log(0.1), math.log(10.0))), 0.1, 10.0)
    eigen_z = jnp.clip(jnp.exp(jax.random.uniform(keys[6], (NZ,), jnp.float32, math.log(0.1), math.log(10.0))), 0.1, 10.0)
    return {"source": source, "basis_x": basis_x, "basis_y": basis_y, "basis_z": basis_z, "eigen_x": eigen_x, "eigen_y": eigen_y, "eigen_z": eigen_z}


HIGH = lax.Precision.HIGHEST


def reference(source, basis_x, basis_y, basis_z, eigen_x, eigen_y, eigen_z):
    field = jnp.einsum('ai,abc->ibc', basis_x, source, precision=HIGH)
    field = jnp.einsum('bj,ibc->ijc', basis_y, field, precision=HIGH)
    field = jnp.einsum('ck,ijc->ijk', basis_z, field, precision=HIGH)
    denom = eigen_x[:, None, None] + eigen_y[None, :, None] + eigen_z[None, None, :]
    field = field / denom
    field = jnp.einsum('ck,ijk->ijc', basis_z, field, precision=HIGH)
    field = jnp.einsum('bj,ijc->ibc', basis_y, field, precision=HIGH)
    field = jnp.einsum('ai,ibc->abc', basis_x, field, precision=HIGH)
    return field
```

```python
import functools

import jax
import jax.numpy as jnp
from jax import lax
from jax.experimental import pallas as pl
from jax.experimental.layout import Layout, with_layout_constraint
from jax.experimental.pallas import tpu as pltpu
from jax.sharding import PartitionSpec as P

FAST = lax.Precision.HIGH
FULL = lax.Precision.HIGHEST
MESH = pl.DeviceIdType.MESH
LANES = 128
SUB = 8
LIMIT = 46 << 20
OUT_SHAPE = pltpu.VMEM


def split(value):
    high = value.astype(jnp.bfloat16)
    low = (value - high.astype(jnp.float32)).astype(jnp.bfloat16)
    return high, low


def product(left, right, dims=((1,), (0,))):
    dot = functools.partial(
        lax.dot_general, dimension_numbers=(dims, ((), ())), preferred_element_type=jnp.float32
    )
    (lh, ll), (rh, rl) = left, right
    return dot(lh, rh) + (dot(lh, rl) + dot(ll, rh))


def partners(rows_n, cols_n):
    half = cols_n // 2
    near, far = list(range(half)), list(range(half, cols_n))
    return [(r, c) for r in range(rows_n) for c in far] + [
        (r, c) for r in range(rows_n) for c in reversed(near)
    ]


def fused(
    rows_n, cols_n,
    source, basis_x, basis_y, basis_z, eigen_x, eigen_y, eigen_z,
    out,
    stage, arrived, z_high, z_low, x_high, x_low, xt_high, xt_low, y_high, y_low, yt_high, yt_low,
    exy, load_sem, basis_sem, send1, recv1, send2, recv2, credit,
):
    ax, by, nz = source.shape
    devices = rows_n * cols_n
    planes, _, nx, _ = stage.shape
    chunks, groups = planes // SUB, ax // SUB
    part = devices * SUB
    row, col = lax.axis_index("row"), lax.axis_index("col")
    me = row * cols_n + col
    order = partners(rows_n, cols_n)
    stage_flat = stage.reshape(planes * cols_n * nx, by)
    arrived_flat = arrived.reshape(planes * cols_n * nx, by)
    lines = arrived.reshape(chunks, devices, SUB, ax, by)
    chunk_rows = SUB * cols_n * nx

    def load(step, slot):
        g = lax.rem(step, groups)
        return pltpu.make_async_copy(
            source.at[pl.ds(g * SUB, SUB)], out.at[pl.ds(slot * SUB, SUB)], load_sem.at[slot]
        )

    side = nx // by

    def basis_at(n):
        return pl.ds(2 * SUB + n * side, side)

    def basis_copy(ref, n):
        return pltpu.make_async_copy(ref.reshape(side, by, ref.shape[1]), out.at[basis_at(n)], basis_sem.at[n])

    basis_copy(basis_z, 0).start()
    load(0, 0).start()
    load(1, 1).start()
    basis_copy(basis_x, 1).start()
    basis_copy(basis_y, 2).start()

    barrier = pltpu.get_barrier_semaphore()
    for r, c in order:
        if r or c:
            pl.semaphore_signal(barrier, inc=1, device_id=(row ^ r, col ^ c), device_id_type=MESH)

    basis_copy(basis_z, 0).wait()
    turned = out[basis_at(0)].reshape(nz, nz).T
    for h in range(chunks):
        rows = [turned[d * planes + h * SUB :][:SUB] for d in range(devices)]
        z_high[h], z_low[h] = split(jnp.concatenate(rows, axis=0))

    def exchange(make_src, make_dst, send_sem, recv_sem):
        for r, c in order:
            r2, c2 = row ^ r, col ^ c
            if r or c:
                pltpu.make_async_remote_copy(
                    src_ref=make_src(r2, c2), dst_ref=make_dst(), send_sem=send_sem,
                    recv_sem=recv_sem, device_id=(r2, c2), device_id_type=MESH,
                ).start()
            else:
                pltpu.make_async_copy(make_src(r2, c2), make_dst(), recv_sem).start()

    def block(ref, h, r, c, g):
        start = pl.multiple_of(r * ax + g * SUB, SUB)
        return ref.at[pl.ds(h * SUB, SUB), c, pl.ds(start, SUB), :]

    def wait_rows(ref, count, sem):
        view = ref.at[pl.ds(0, count)]
        pltpu.make_async_copy(view, view, sem).wait()

    pl.semaphore_wait(barrier, devices - 1)

    @pl.loop(0, chunks * groups)
    def _(step):
        h, g, slot = step // groups, lax.rem(step, groups), lax.rem(step, 2)
        load(step, slot).wait()

        @pl.loop(0, SUB // 2)
        def _(pair):
            a = pair * 2
            lhs = (z_high[h], z_low[h])
            rhs = split(out[pl.ds(slot * SUB + a, 2)].reshape(2 * by, nz))
            field = product(lhs, rhs, ((1,), (1,)))
            for n in range(2):
                for d in range(devices):
                    start = h * chunk_rows + (d % cols_n) * nx + (d // cols_n) * ax + g * SUB + a + n
                    stage_flat[pl.ds(start, SUB, stride=cols_n * nx), :] = field[
                        d * SUB : (d + 1) * SUB, n * by : (n + 1) * by
                    ]

        @pl.when(step + 2 < chunks * groups)
        def _():
            load(step + 2, slot).start()

        exchange(
            lambda r, c: block(stage, h, r, c, g),
            lambda: block(arrived, h, row, col, g),
            send1.at[h], recv1.at[h],
        )

    basis_copy(basis_x, 1).wait()
    basis_copy(basis_y, 2).wait()
    for n, natural, turned_refs in ((1, (x_high, x_low), (xt_high, xt_low)), (2, (y_high, y_low), (yt_high, yt_low))):
        value = out[basis_at(n)].reshape(nx, nx)
        natural[0][...], natural[1][...] = split(value)
        turned_refs[0][...], turned_refs[1][...] = split(value.T)
    exy[...] = jnp.broadcast_to(eigen_x[...], exy.shape).T + eigen_y[...]

    def both(pair):
        return pair[0][...], pair[1][...]

    for h in range(chunks):
        wait_rows(arrived_flat, chunk_rows, recv1.at[h])
        wait_rows(stage_flat, (devices - 1) * SUB * ax, send1.at[h])

        @pl.loop(h * SUB, (h + 1) * SUB)
        def _(p):
            field = jnp.concatenate([arrived[p, c] for c in range(cols_n)], axis=1)
            field = product(both((xt_high, xt_low)), split(field))
            field = product(split(field), both((y_high, y_low)))
            field = field / (exy[...] + eigen_z[me * planes + p])
            field = product(split(field), both((yt_high, yt_low)))
            field = product(both((x_high, x_low)), split(field))
            for c in range(cols_n):
                stage[p, c] = field[:, c * by : (c + 1) * by]

        for r, c in order:
            if r or c:
                pl.semaphore_signal(credit.at[h], inc=1, device_id=(row ^ r, col ^ c), device_id_type=MESH)
        pl.semaphore_wait(credit.at[h], devices - 1)

        @pl.loop(0, groups)
        def _(g):
            exchange(
                lambda r, c: block(stage, h, r, c, g),
                lambda: lines.at[h, me, :, pl.ds(g * SUB, SUB), :],
                send2.at[h], recv2.at[h, g],
            )

    for h in range(chunks):

        @pl.loop(0, groups)
        def _(g):
            wait_rows(arrived_flat, part * SUB, recv2.at[h, g])

            @pl.loop(0, SUB // 2)
            def _(pair):
                a = g * SUB + pair * 2
                sides = [
                    arrived_flat[pl.ds(h * chunk_rows + a + n, part, stride=ax), :].T for n in range(2)
                ]
                lhs = split(jnp.concatenate(sides, axis=0))
                field = product(lhs, (z_high[h], z_low[h])).reshape(2, by, nz)
                if h:
                    out[pl.ds(a, 2)] += field
                else:
                    out[pl.ds(a, 2)] = field

    for h in range(chunks):
        wait_rows(stage_flat, (devices - 1) * SUB * ax, send2.at[h])


def fused_local(source, basis_x, basis_y, basis_z, eigen_x, eigen_y, eigen_z):
    rows_n, cols_n = lax.axis_size("row"), lax.axis_size("col")
    devices = rows_n * cols_n
    ax, by, nz = source.shape
    nx, ny = basis_x.shape[0], basis_y.shape[0]
    planes = nz // devices
    chunks, groups = planes // SUB, ax // SUB
    dma, any_space = pltpu.SemaphoreType.DMA, pl.BlockSpec(memory_space=pl.ANY)
    vmem, smem = pl.BlockSpec(memory_space=pltpu.VMEM), pl.BlockSpec(memory_space=pltpu.SMEM)
    field = pltpu.VMEM((planes, cols_n, nx, by), jnp.float32)
    zb = pltpu.VMEM((chunks, devices * SUB, nz), jnp.bfloat16)
    xb = pltpu.VMEM((nx, nx), jnp.bfloat16)
    yb = pltpu.VMEM((ny, ny), jnp.bfloat16)
    result = pl.pallas_call(
        functools.partial(fused, rows_n, cols_n),
        out_shape=OUT_SHAPE((ax, by, nz), jnp.float32),
        in_specs=[any_space] * 4 + [vmem, vmem, smem],
        out_specs=vmem,
        scratch_shapes=[
            field, field, zb, zb, xb, xb, xb, xb, yb, yb, yb, yb,
            pltpu.VMEM((nx, ny), jnp.float32),
            dma((2,)), dma((3,)), dma((chunks,)), dma((chunks,)), dma((chunks,)), dma((chunks, groups)),
            pltpu.SemaphoreType.REGULAR((chunks,)),
        ],
        compiler_params=pltpu.CompilerParams(
            collective_id=0, has_side_effects=True, vmem_limit_bytes=LIMIT
        ),
    )(source, basis_x, basis_y, basis_z, eigen_x[None], eigen_y[None], eigen_z)
    return result


def cuts(planes):
    if planes < 3:
        return [(p, 1) for p in range(planes)]
    first = max(1, planes * 2 // 16)
    last = max(1, planes * 6 // 16)
    return [(0, first), (first, planes - first - last), (planes - last, last)]


def staged_local(source, basis_x, basis_y, basis_z, eigen_x, eigen_y, eigen_z):
    rows_n = lax.axis_size("row")
    cols_n = lax.axis_size("col")
    devices = rows_n * cols_n
    me = lax.axis_index("row") * cols_n + lax.axis_index("col")
    ax, by, nz = source.shape
    nx, ny = basis_x.shape[0], basis_y.shape[0]
    planes = nz // devices
    bz = basis_z.reshape(nz, devices, planes)
    ez = lax.dynamic_slice_in_dim(eigen_z, me * planes, planes, 0)
    exy = eigen_x[:, None] + eigen_y[None, :]
    pieces = cuts(planes)

    def columns(piece):
        start, count = piece
        return bz[:, :, start : start + count].reshape(nz, devices * count)

    def exchange(field):
        return lax.all_to_all(field, ("row", "col"), split_axis=0, concat_axis=0, tiled=True)

    def forward(piece):
        field = jnp.einsum("ck,abc->kab", columns(piece), source, precision=FAST)
        return with_layout_constraint(field, Layout(major_to_minor=(0, 1, 2)))

    def middle(piece, field):
        start, count = piece
        field = field.reshape(rows_n, cols_n, count, ax, by)
        field = field.transpose(2, 0, 3, 1, 4).reshape(count, nx, ny)
        field = jnp.einsum("xi,kxy->kiy", basis_x, field, precision=FULL)
        field = jnp.einsum("kiy,yj->kij", field, basis_y, precision=FULL)
        field = field / (exy[None] + ez[start : start + count][:, None, None])
        field = jnp.einsum("kij,yj->kiy", field, basis_y, precision=FULL)
        field = jnp.einsum("xi,kiy->kxy", basis_x, field, precision=FULL)
        field = field.reshape(count, rows_n, ax, cols_n, by).transpose(1, 3, 0, 2, 4)
        return field.reshape(devices * count, ax, by)

    def backward(piece, field, precision):
        return jnp.einsum("ck,kab->abc", columns(piece), field, precision=precision)

    count = len(pieces)
    tie = lax.optimization_barrier
    fields = [forward(pieces[0])]
    arrived = [exchange(fields[0])]
    done = []
    for n in range(1, count):
        field = forward(pieces[n])
        if done:
            arrived[-1], field, done[-1] = tie((arrived[-1], field, done[-1]))
        else:
            arrived[-1], field = tie((arrived[-1], field))
        arrived.append(exchange(field))
        done.append(middle(pieces[n - 1], arrived[n - 1]))
    if done:
        arrived[-1], *done = tie((arrived[-1], *done))
    returned = []
    for n, piece in enumerate(pieces):
        if n == count - 1:
            if count > 2:
                returned[0], arrived[-1] = tie((returned[0], arrived[-1]))
            done.append(middle(piece, arrived[-1]))
        field = done[n]
        if returned:
            returned[-1], field = tie((returned[-1], field))
        returned.append(exchange(field))
    total = backward(pieces[0], returned[0], FULL)
    for piece, field in zip(pieces[1:], returned[1:]):
        total = lax.optimization_barrier(total)
        last = piece is pieces[-1]
        total = total + backward(piece, field, FAST if last else FULL)
    return total


def solution(mesh):
    rows_n, cols_n = mesh.shape["row"], mesh.shape["col"]

    def local(source, basis_x, basis_y, basis_z, *eigen):
        ax, by, nz = source.shape
        square = basis_x.shape == basis_y.shape == basis_z.shape
        planes = nz // (rows_n * cols_n)
        power = not (rows_n & (rows_n - 1) or cols_n & (cols_n - 1))
        fits = by == LANES and ax % SUB == 0 and planes % SUB == 0
        body = fused_local if square and power and fits else staged_local
        return body(source, basis_x, basis_y, basis_z, *eigen)

    placed = (P("row", "col", None), P(), P(), P(), P(), P(), P())
    return jax.shard_map(
        local, mesh=mesh, in_specs=placed, out_specs=P("row", "col", None), check_vma=False
    )
```

```python
import functools

import jax
import jax.numpy as jnp
from jax import lax
from jax.experimental import pallas as pl
from jax.experimental.layout import Layout, with_layout_constraint
from jax.experimental.pallas import tpu as pltpu
from jax.sharding import PartitionSpec as P

FAST = lax.Precision.HIGH
FULL = lax.Precision.HIGHEST
MESH = pl.DeviceIdType.MESH
LANES = 128
SUB = 8
LIMIT = 45 << 20
TAIL_LIMIT = 20 << 20


def split(value):
    high = value.astype(jnp.bfloat16)
    low = (value - high.astype(jnp.float32)).astype(jnp.bfloat16)
    return high, low


def product(left, right, dims=((1,), (0,))):
    dot = functools.partial(
        lax.dot_general, dimension_numbers=(dims, ((), ())), preferred_element_type=jnp.float32
    )
    (lh, ll), (rh, rl) = left, right
    return dot(lh, rh) + (dot(lh, rl) + dot(ll, rh))


def partners(rows_n, cols_n):
    half = cols_n // 2
    near, far = list(range(half)), list(range(half, cols_n))
    return [(r, c) for r in range(rows_n) for c in far] + [
        (r, c) for r in range(rows_n) for c in reversed(near)
    ]


def fused(
    rows_n, cols_n,
    source, basis_x, basis_y, basis_z, eigen_x, eigen_y, eigen_z,
    out, last, z_high, z_low,
    stage, arrived, x_high, x_low, xt_high, xt_low, y_high, y_low, yt_high, yt_low,
    exy, ex, ey, ez, eigen_sem, load_sem, basis_sem, send1, recv1, send2, recv2, credit,
):
    ax, by, nz = source.shape
    devices = rows_n * cols_n
    planes, _, nx, _ = stage.shape
    chunks, groups = planes // SUB, ax // SUB
    part = devices * SUB
    row, col = lax.axis_index("row"), lax.axis_index("col")
    me = row * cols_n + col
    order = partners(rows_n, cols_n)
    stage_flat = stage.reshape(planes * cols_n * nx, by)
    arrived_flat = arrived.reshape(planes * cols_n * nx, by)
    lines = arrived.reshape(chunks, devices, SUB, ax, by)
    chunk_rows = SUB * cols_n * nx

    def load(step, slot):
        g = lax.rem(step, groups)
        return pltpu.make_async_copy(
            source.at[pl.ds(g * SUB, SUB)], out.at[pl.ds(slot * SUB, SUB)], load_sem.at[slot]
        )

    side = nx // by

    def basis_at(n):
        return pl.ds(2 * SUB + n * side, side)

    def basis_copy(ref, n):
        return pltpu.make_async_copy(ref.reshape(side, by, ref.shape[1]), out.at[basis_at(n)], basis_sem.at[n])

    eigen = [(eigen_x, ex.at[0]), (eigen_y, ey.at[0]), (eigen_z, ez)]
    eigen = [pltpu.make_async_copy(a, b, eigen_sem.at[n]) for n, (a, b) in enumerate(eigen)]

    basis_copy(basis_z, 0).start()
    load(0, 0).start()
    barrier = pltpu.get_barrier_semaphore()
    for r, c in order:
        if r or c:
            pl.semaphore_signal(barrier, inc=1, device_id=(row ^ r, col ^ c), device_id_type=MESH)

    def choose(h):
        turned = out[basis_at(3)].reshape(nz, nz)
        rows = [turned[d * planes + h * SUB :][:SUB] for d in range(devices)]
        z_high[h], z_low[h] = split(jnp.concatenate(rows, axis=0))

    basis_copy(basis_z, 0).wait()
    out[basis_at(3)] = out[basis_at(0)].reshape(nz, nz).T.reshape(side, by, nz)
    choose(0)

    def exchange(make_src, make_dst, send_sem, recv_sem):
        for r, c in order:
            r2, c2 = row ^ r, col ^ c
            if r or c:
                pltpu.make_async_remote_copy(
                    src_ref=make_src(r2, c2), dst_ref=make_dst(), send_sem=send_sem,
                    recv_sem=recv_sem, device_id=(r2, c2), device_id_type=MESH,
                ).start()
            else:
                pltpu.make_async_copy(make_src(r2, c2), make_dst(), recv_sem).start()

    def block(ref, h, r, c, g):
        start = pl.multiple_of(r * ax + g * SUB, SUB)
        return ref.at[pl.ds(h * SUB, SUB), c, pl.ds(start, SUB), :]

    def wait_rows(ref, count, sem):
        view = ref.at[pl.ds(0, count)]
        pltpu.make_async_copy(view, view, sem).wait()

    def forward(step):
        h, g, slot = step // groups, lax.rem(step, groups), lax.rem(step, 2)
        load(step, slot).wait()
        lhs = (z_high[h], z_low[h])
        rhs = split(out[pl.ds(slot * SUB, SUB)].reshape(SUB * by, nz))
        field = product(lhs, rhs, ((1,), (1,)))
        for n in range(SUB):
            for d in range(devices):
                start = h * chunk_rows + (d % cols_n) * nx + (d // cols_n) * ax + g * SUB + n
                stage_flat[pl.ds(start, SUB, stride=cols_n * nx), :] = field[
                    d * SUB : (d + 1) * SUB, n * by : (n + 1) * by
                ]

    def send_forward(step):
        h, g = step // groups, lax.rem(step, groups)
        exchange(
            lambda r, c: block(stage, h, r, c, g),
            lambda: block(arrived, h, row, col, g),
            send1.at[h], recv1.at[h],
        )

    start = jnp.int32(0)
    forward(start)
    pl.semaphore_wait(barrier, devices - 1)
    send_forward(start)
    load(1, 1).start()
    load(2, 0).start()
    basis_copy(basis_x, 1).start()
    basis_copy(basis_y, 2).start()
    for copy in eigen:
        copy.start()
    for h in range(1, chunks):
        choose(h)

    @pl.loop(1, chunks * groups)
    def _(step):
        forward(step)
        send_forward(step)

        @pl.when(step + 2 < chunks * groups)
        def _():
            load(step + 2, lax.rem(step, 2)).start()

    basis_copy(basis_x, 1).wait()
    basis_copy(basis_y, 2).wait()
    for n, natural, turned_refs in ((1, (x_high, x_low), (xt_high, xt_low)), (2, (y_high, y_low), (yt_high, yt_low))):
        value = out[basis_at(n)].reshape(nx, nx)
        natural[0][...], natural[1][...] = split(value)
        turned_refs[0][...], turned_refs[1][...] = split(value.T)
    for copy in eigen:
        copy.wait()
    exy[...] = jnp.broadcast_to(ex[...], exy.shape).T + ey[...]

    def both(pair):
        return pair[0][...], pair[1][...]

    for h in range(chunks):
        wait_rows(arrived_flat, chunk_rows, recv1.at[h])
        wait_rows(stage_flat, (devices - 1) * SUB * ax, send1.at[h])

        @pl.loop(h * SUB, (h + 1) * SUB)
        def _(p):
            field = jnp.concatenate([arrived[p, c] for c in range(cols_n)], axis=1)
            field = product(both((xt_high, xt_low)), split(field))
            field = product(split(field), both((y_high, y_low)))
            field = field / (exy[...] + ez[me * planes + p])
            field = product(split(field), both((yt_high, yt_low)))
            field = product(both((x_high, x_low)), split(field))
            for c in range(cols_n):
                stage[p, c] = field[:, c * by : (c + 1) * by]

        for r, c in order:
            if r or c:
                pl.semaphore_signal(credit.at[h], inc=1, device_id=(row ^ r, col ^ c), device_id_type=MESH)
        pl.semaphore_wait(credit.at[h], devices - 1)

        @pl.loop(0, groups)
        def _(g):
            exchange(
                lambda r, c: block(stage, h, r, c, g),
                lambda: lines.at[h, me, :, pl.ds(g * SUB, SUB), :],
                send2.at[h], recv2.at[h, g],
            )

    for h in range(chunks):

        @pl.loop(0, groups - (h == chunks - 1))
        def _(g):
            wait_rows(arrived_flat, part * SUB, recv2.at[h, g])
            a = g * SUB
            sides = [
                arrived_flat[pl.ds(h * chunk_rows + a + n, part, stride=ax), :].T for n in range(SUB)
            ]
            field = backward(sides, z_high[h], z_low[h])
            if h:
                field = field + out[pl.ds(a, SUB)]
            out[pl.ds(a, SUB)] = field

    h, g = chunks - 1, groups - 1
    wait_rows(arrived_flat, part * SUB, recv2.at[h, g])
    for d in range(devices):
        last[d] = lines[h, d, :, g * SUB :, :]
    for h in range(chunks):
        wait_rows(stage_flat, (devices - 1) * SUB * ax, send2.at[h])


def backward(sides, z_high, z_low):
    field = product(split(jnp.concatenate(sides, axis=0)), (z_high, z_low))
    return field.reshape(len(sides), -1, field.shape[1])


def finish(most, last, z_high, z_low, out, tail, sems):
    groups = out.shape[0] // SUB
    copies = [
        pltpu.make_async_copy(most.at[pl.ds(g * SUB, SUB)], out.at[pl.ds(g * SUB, SUB)], sems.at[g])
        for g in range(groups - 1)
    ]
    copies.append(pltpu.make_async_copy(tail, out.at[pl.ds((groups - 1) * SUB, SUB)], sems.at[groups - 1]))
    for copy in copies[:-1]:
        copy.start()
    part = last.shape[0] * SUB
    rows = last.reshape(part * SUB, last.shape[3])
    sides = [rows[pl.ds(n, part, stride=SUB), :].T for n in range(SUB)]
    field = backward(sides, z_high[z_high.shape[0] - 1], z_low[z_low.shape[0] - 1])
    tail[...] = field + most[pl.ds((groups - 1) * SUB, SUB)]
    copies[-1].start()
    for copy in copies:
        copy.wait()


def fused_local(source, basis_x, basis_y, basis_z, eigen_x, eigen_y, eigen_z):
    rows_n, cols_n = lax.axis_size("row"), lax.axis_size("col")
    devices = rows_n * cols_n
    ax, by, nz = source.shape
    nx, ny = basis_x.shape[0], basis_y.shape[0]
    planes = nz // devices
    chunks, groups = planes // SUB, ax // SUB
    dma, any_space = pltpu.SemaphoreType.DMA, pl.BlockSpec(memory_space=pl.ANY)
    vmem = pl.BlockSpec(memory_space=pltpu.VMEM)
    field = pltpu.VMEM((planes, cols_n, nx, by), jnp.float32)
    zb = pltpu.VMEM((chunks, devices * SUB, nz), jnp.bfloat16)
    xb = pltpu.VMEM((nx, nx), jnp.bfloat16)
    yb = pltpu.VMEM((ny, ny), jnp.bfloat16)
    results = pl.pallas_call(
        functools.partial(fused, rows_n, cols_n),
        out_shape=(
            pltpu.VMEM((ax, by, nz), jnp.float32), pltpu.VMEM((devices, SUB, SUB, by), jnp.float32), zb, zb,
        ),
        in_specs=[any_space] * 7,
        out_specs=(vmem,) * 4,
        scratch_shapes=[
            field, field, xb, xb, xb, xb, yb, yb, yb, yb,
            pltpu.VMEM((nx, ny), jnp.float32), pltpu.VMEM((1, nx), jnp.float32), pltpu.VMEM((1, ny), jnp.float32),
            pltpu.SMEM((nz,), jnp.float32),
            dma((3,)), dma((2,)), dma((3,)), dma((chunks,)), dma((chunks,)), dma((chunks,)), dma((chunks, groups)),
            pltpu.SemaphoreType.REGULAR((chunks,)),
        ],
        compiler_params=pltpu.CompilerParams(
            collective_id=0, has_side_effects=True, vmem_limit_bytes=LIMIT
        ),
    )(source, basis_x, basis_y, basis_z, eigen_x, eigen_y, eigen_z)
    return pl.pallas_call(
        finish,
        out_shape=jax.ShapeDtypeStruct((ax, by, nz), jnp.float32),
        in_specs=[vmem] * 4,
        out_specs=any_space,
        scratch_shapes=[pltpu.VMEM((SUB, by, nz), jnp.float32), dma((groups,))],
        compiler_params=pltpu.CompilerParams(vmem_limit_bytes=TAIL_LIMIT),
    )(*results)


def cuts(planes):
    if planes < 3:
        return [(p, 1) for p in range(planes)]
    first = max(1, planes * 2 // 16)
    last = max(1, planes * 6 // 16)
    return [(0, first), (first, planes - first - last), (planes - last, last)]


def staged_local(source, basis_x, basis_y, basis_z, eigen_x, eigen_y, eigen_z):
    rows_n = lax.axis_size("row")
    cols_n = lax.axis_size("col")
    devices = rows_n * cols_n
    me = lax.axis_index("row") * cols_n + lax.axis_index("col")
    ax, by, nz = source.shape
    nx, ny = basis_x.shape[0], basis_y.shape[0]
    planes = nz // devices
    bz = basis_z.reshape(nz, devices, planes)
    ez = lax.dynamic_slice_in_dim(eigen_z, me * planes, planes, 0)
    exy = eigen_x[:, None] + eigen_y[None, :]
    pieces = cuts(planes)

    def columns(piece):
        start, count = piece
        return bz[:, :, start : start + count].reshape(nz, devices * count)

    def exchange(field):
        return lax.all_to_all(field, ("row", "col"), split_axis=0, concat_axis=0, tiled=True)

    def forward(piece):
        field = jnp.einsum("ck,abc->kab", columns(piece), source, precision=FAST)
        return with_layout_constraint(field, Layout(major_to_minor=(0, 1, 2)))

    def middle(piece, field):
        start, count = piece
        field = field.reshape(rows_n, cols_n, count, ax, by)
        field = field.transpose(2, 0, 3, 1, 4).reshape(count, nx, ny)
        field = jnp.einsum("xi,kxy->kiy", basis_x, field, precision=FULL)
        field = jnp.einsum("kiy,yj->kij", field, basis_y, precision=FULL)
        field = field / (exy[None] + ez[start : start + count][:, None, None])
        field = jnp.einsum("kij,yj->kiy", field, basis_y, precision=FULL)
        field = jnp.einsum("xi,kiy->kxy", basis_x, field, precision=FULL)
        field = field.reshape(count, rows_n, ax, cols_n, by).transpose(1, 3, 0, 2, 4)
        return field.reshape(devices * count, ax, by)

    def backward(piece, field, precision):
        return jnp.einsum("ck,kab->abc", columns(piece), field, precision=precision)

    count = len(pieces)
    tie = lax.optimization_barrier
    fields = [forward(pieces[0])]
    arrived = [exchange(fields[0])]
    done = []
    for n in range(1, count):
        field = forward(pieces[n])
        if done:
            arrived[-1], field, done[-1] = tie((arrived[-1], field, done[-1]))
        else:
            arrived[-1], field = tie((arrived[-1], field))
        arrived.append(exchange(field))
        done.append(middle(pieces[n - 1], arrived[n - 1]))
    if done:
        arrived[-1], *done = tie((arrived[-1], *done))
    returned = []
    for n, piece in enumerate(pieces):
        if n == count - 1:
            if count > 2:
                returned[0], arrived[-1] = tie((returned[0], arrived[-1]))
            done.append(middle(piece, arrived[-1]))
        field = done[n]
        if returned:
            returned[-1], field = tie((returned[-1], field))
        returned.append(exchange(field))
    total = backward(pieces[0], returned[0], FULL)
    for piece, field in zip(pieces[1:], returned[1:]):
        total = lax.optimization_barrier(total)
        last = piece is pieces[-1]
        total = total + backward(piece, field, FAST if last else FULL)
    return total


def solution(mesh):
    rows_n, cols_n = mesh.shape["row"], mesh.shape["col"]

    def local(source, basis_x, basis_y, basis_z, *eigen):
        ax, by, nz = source.shape
        square = basis_x.shape == basis_y.shape == basis_z.shape
        planes = nz // (rows_n * cols_n)
        power = not (rows_n & (rows_n - 1) or cols_n & (cols_n - 1))
        fits = by == LANES and nz * ax >= 4 * SUB * SUB * rows_n * cols_n and ax % SUB == 0 and planes % SUB == 0
        body = fused_local if square and power and fits else staged_local
        return body(source, basis_x, basis_y, basis_z, *eigen)

    placed = (P("row", "col", None), P(), P(), P(), P(), P(), P())
    return jax.shard_map(
        local, mesh=mesh, in_specs=placed, out_specs=P("row", "col", None), check_vma=False
    )
```

```python
import functools

import jax
import jax.numpy as jnp
from jax import lax
from jax.experimental import pallas as pl
from jax.experimental.layout import Layout, with_layout_constraint
from jax.experimental.pallas import tpu as pltpu
from jax.sharding import PartitionSpec as P

FAST = lax.Precision.HIGH
FULL = lax.Precision.HIGHEST
MESH = pl.DeviceIdType.MESH
LANES = 128
SUB = 8
LIMIT = 45 << 20
TAIL_LIMIT = 20 << 20


def split(value):
    high = value.astype(jnp.bfloat16)
    low = (value - high.astype(jnp.float32)).astype(jnp.bfloat16)
    return high, low


def product(left, right, dims=((1,), (0,))):
    dot = functools.partial(
        lax.dot_general, dimension_numbers=(dims, ((), ())), preferred_element_type=jnp.float32
    )
    (lh, ll), (rh, rl) = left, right
    return dot(lh, rh) + (dot(lh, rl) + dot(ll, rh))


def partners(rows_n, cols_n):
    half = cols_n // 2
    near, far = list(range(half)), list(range(half, cols_n))
    return [(r, c) for r in range(rows_n) for c in far] + [
        (r, c) for r in range(rows_n) for c in reversed(near)
    ]


def fused(
    rows_n, cols_n,
    source, basis_x, basis_y, basis_z, eigen_x, eigen_y, eigen_z,
    out, last, z_high, z_low,
    stage, arrived, x_high, x_low, xt_high, xt_low, y_high, y_low, yt_high, yt_low,
    exy, ex, ey, ez, eigen_sem, load_sem, basis_sem, send1, recv1, send2, recv2, credit,
):
    ax, by, nz = source.shape
    devices = rows_n * cols_n
    planes, _, nx, _ = stage.shape
    chunks, groups = planes // SUB, ax // SUB
    part = devices * SUB
    row, col = lax.axis_index("row"), lax.axis_index("col")
    me = row * cols_n + col
    order = partners(rows_n, cols_n)
    stage_flat = stage.reshape(planes * cols_n * nx, by)
    arrived_flat = arrived.reshape(planes * cols_n * nx, by)
    lines = arrived.reshape(chunks, devices, SUB, ax, by)
    chunk_rows = SUB * cols_n * nx

    side, depth = nx // by, (ax - 4 * (nx // by)) // SUB

    def slot_at(step):
        return pl.ds(4 * side + lax.rem(step, depth) * SUB, SUB)

    def load(step):
        rows = pl.ds(lax.rem(step, groups) * SUB, SUB)
        return pltpu.make_async_copy(source.at[rows], out.at[slot_at(step)], load_sem.at[lax.rem(step, depth)])

    def basis_at(n):
        return pl.ds(n * side, side)

    def basis_copy(ref, n):
        return pltpu.make_async_copy(ref.reshape(side, by, ref.shape[1]), out.at[basis_at(n)], basis_sem.at[n])

    eigen = [(eigen_x, ex.at[0]), (eigen_y, ey.at[0]), (eigen_z, ez)]
    eigen = [pltpu.make_async_copy(a, b, eigen_sem.at[n]) for n, (a, b) in enumerate(eigen)]

    basis_copy(basis_z, 0).start()
    load(jnp.int32(0)).start()
    barrier = pltpu.get_barrier_semaphore()
    for r, c in order:
        if r or c:
            pl.semaphore_signal(barrier, inc=1, device_id=(row ^ r, col ^ c), device_id_type=MESH)

    def choose(h):
        turned = out[basis_at(3)].reshape(nz, nz)
        rows = [turned[d * planes + h * SUB :][:SUB] for d in range(devices)]
        z_high[h], z_low[h] = split(jnp.concatenate(rows, axis=0))

    basis_copy(basis_z, 0).wait()
    out[basis_at(3)] = out[basis_at(0)].reshape(nz, nz).T.reshape(side, by, nz)
    for n in range(1, depth):
        load(jnp.int32(n)).start()
    choose(0)

    def exchange(make_src, make_dst, send_sem, recv_sem, offsets=order):
        for r, c in offsets:
            r2, c2 = row ^ r, col ^ c
            if r or c:
                pltpu.make_async_remote_copy(
                    src_ref=make_src(r2, c2), dst_ref=make_dst(), send_sem=send_sem,
                    recv_sem=recv_sem, device_id=(r2, c2), device_id_type=MESH,
                ).start()
            else:
                pltpu.make_async_copy(make_src(r2, c2), make_dst(), recv_sem).start()

    def block(ref, h, r, c, g):
        start = pl.multiple_of(r * ax + g * SUB, SUB)
        return ref.at[pl.ds(h * SUB, SUB), c, pl.ds(start, SUB), :]

    def wait_rows(ref, count, sem):
        view = ref.at[pl.ds(0, count)]
        pltpu.make_async_copy(view, view, sem).wait()

    def forward(step):
        h, g = step // groups, lax.rem(step, groups)
        load(step).wait()
        lhs = (z_high[h], z_low[h])
        rhs = split(out[slot_at(step)].reshape(SUB * by, nz))
        field = product(lhs, rhs, ((1,), (1,)))
        for n in range(SUB):
            for d in range(devices):
                start = h * chunk_rows + (d % cols_n) * nx + (d // cols_n) * ax + g * SUB + n
                stage_flat[pl.ds(start, SUB, stride=cols_n * nx), :] = field[
                    d * SUB : (d + 1) * SUB, n * by : (n + 1) * by
                ]
        pl.when(step + depth < chunks * groups)(lambda: load(step + depth).start())

    def send_forward(step):
        h, g = step // groups, lax.rem(step, groups)
        exchange(
            lambda r, c: block(stage, h, r, c, g),
            lambda: block(arrived, h, row, col, g),
            send1.at[h], recv1.at[h],
        )

    start = jnp.int32(0)
    forward(start)
    pl.semaphore_wait(barrier, devices - 1)
    send_forward(start)
    basis_copy(basis_x, 1).start()
    basis_copy(basis_y, 2).start()
    for copy in eigen:
        copy.start()
    for h in range(1, chunks):
        choose(h)

    @pl.loop(1, chunks * groups)
    def _(step):
        forward(step)
        send_forward(step)

    basis_copy(basis_x, 1).wait()
    basis_copy(basis_y, 2).wait()
    for n, natural, turned_refs in ((1, (x_high, x_low), (xt_high, xt_low)), (2, (y_high, y_low), (yt_high, yt_low))):
        value = out[basis_at(n)].reshape(nx, nx)
        natural[0][...], natural[1][...] = split(value)
        turned_refs[0][...], turned_refs[1][...] = split(value.T)
    for copy in eigen:
        copy.wait()
    exy[...] = jnp.broadcast_to(ex[...], exy.shape).T + ey[...]

    def both(pair):
        return pair[0][...], pair[1][...]

    for h in range(chunks):
        wait_rows(arrived_flat, chunk_rows, recv1.at[h])
        wait_rows(stage_flat, (devices - 1) * SUB * ax, send1.at[h])

        @pl.loop(h * SUB, (h + 1) * SUB)
        def _(p):
            field = jnp.concatenate([arrived[p, c] for c in range(cols_n)], axis=1)
            field = product(both((xt_high, xt_low)), split(field))
            field = product(split(field), both((y_high, y_low)))
            field = field / (exy[...] + ez[me * planes + p])
            field = product(split(field), both((yt_high, yt_low)))
            field = product(both((x_high, x_low)), split(field))
            for c in range(cols_n):
                stage[p, c] = field[:, c * by : (c + 1) * by]

        for r, c in order:
            if r or c:
                pl.semaphore_signal(credit.at[h], inc=1, device_id=(row ^ r, col ^ c), device_id_type=MESH)
        pl.semaphore_wait(credit.at[h], devices - 1)

        def send_back(g, offsets=order):
            exchange(
                lambda r, c: block(stage, h, r, c, g),
                lambda: lines.at[h, me, :, pl.ds(pl.multiple_of(g * SUB, SUB), SUB), :],
                send2.at[h], recv2.at[h, g], offsets,
            )

        final = h == chunks - 1

        @pl.loop(0, groups - final)
        def _(g):
            send_back(g)

        if final:
            half = cols_n // 2
            columns = [*range(half, cols_n), *reversed(range(half))]
            send_back(groups - 1, [(r, c) for c in columns for r in range(rows_n)])

    for h in range(chunks):

        @pl.loop(0, groups - (h == chunks - 1))
        def _(g):
            wait_rows(arrived_flat, part * SUB, recv2.at[h, g])
            a = g * SUB
            sides = [
                arrived_flat[pl.ds(h * chunk_rows + a + n, part, stride=ax), :].T for n in range(SUB)
            ]
            field = backward(sides, z_high[h], z_low[h])
            if h:
                field = field + out[pl.ds(a, SUB)]
            out[pl.ds(a, SUB)] = field

    h, g = chunks - 1, groups - 1
    wait_rows(arrived_flat, part * SUB, recv2.at[h, g])
    for d in range(devices):
        last[d] = lines[h, d, :, g * SUB :, :]
    for h in range(chunks):
        wait_rows(stage_flat, (devices - 1) * SUB * ax, send2.at[h])


def backward(sides, z_high, z_low):
    field = product(split(jnp.concatenate(sides, axis=0)), (z_high, z_low))
    return field.reshape(len(sides), -1, field.shape[1])


def finish(most, last, z_high, z_low, out, tail, sems):
    start = out.shape[0] - SUB
    step = start // (sems.shape[0] - 1)
    copies = [
        pltpu.make_async_copy(most.at[pl.ds(n * step, step)], out.at[pl.ds(n * step, step)], sems.at[n])
        for n in range(sems.shape[0] - 1)
    ]
    copies.append(pltpu.make_async_copy(tail, out.at[pl.ds(start, SUB)], sems.at[sems.shape[0] - 1]))
    for copy in copies[:-1]:
        copy.start()
    part = last.shape[0] * SUB
    rows = last.reshape(part * SUB, last.shape[3])
    sides = [rows[pl.ds(n, part, stride=SUB), :].T for n in range(SUB)]
    field = backward(sides, z_high[z_high.shape[0] - 1], z_low[z_low.shape[0] - 1])
    tail[...] = field + most[pl.ds(start, SUB)]
    copies[-1].start()
    for copy in copies:
        copy.wait()


def fused_local(source, basis_x, basis_y, basis_z, eigen_x, eigen_y, eigen_z):
    rows_n, cols_n = lax.axis_size("row"), lax.axis_size("col")
    devices = rows_n * cols_n
    ax, by, nz = source.shape
    nx, ny = basis_x.shape[0], basis_y.shape[0]
    planes = nz // devices
    chunks, groups = planes // SUB, ax // SUB
    dma, any_space = pltpu.SemaphoreType.DMA, pl.BlockSpec(memory_space=pl.ANY)
    vmem = pl.BlockSpec(memory_space=pltpu.VMEM)
    field = pltpu.VMEM((planes, cols_n, nx, by), jnp.float32)
    zb = pltpu.VMEM((chunks, devices * SUB, nz), jnp.bfloat16)
    xb = pltpu.VMEM((nx, nx), jnp.bfloat16)
    yb = pltpu.VMEM((ny, ny), jnp.bfloat16)
    results = pl.pallas_call(
        functools.partial(fused, rows_n, cols_n),
        out_shape=(
            pltpu.VMEM((ax, by, nz), jnp.float32), pltpu.VMEM((devices, SUB, SUB, by), jnp.float32), zb, zb,
        ),
        in_specs=[any_space] * 7,
        out_specs=(vmem,) * 4,
        scratch_shapes=[
            field, field, xb, xb, xb, xb, yb, yb, yb, yb,
            pltpu.VMEM((nx, ny), jnp.float32), pltpu.VMEM((1, nx), jnp.float32), pltpu.VMEM((1, ny), jnp.float32),
            pltpu.SMEM((nz,), jnp.float32),
            dma((3,)), dma(((ax - 4 * (nx // by)) // SUB,)), dma((3,)), dma((chunks,)), dma((chunks,)), dma((chunks,)), dma((chunks, groups)),
            pltpu.SemaphoreType.REGULAR((chunks,)),
        ],
        compiler_params=pltpu.CompilerParams(
            collective_id=0, has_side_effects=True, vmem_limit_bytes=LIMIT
        ),
    )(source, basis_x, basis_y, basis_z, eigen_x, eigen_y, eigen_z)
    return pl.pallas_call(
        finish,
        out_shape=jax.ShapeDtypeStruct((ax, by, nz), jnp.float32),
        in_specs=[vmem] * 4,
        out_specs=any_space,
        scratch_shapes=[pltpu.VMEM((SUB, by, nz), jnp.float32), dma((2 * groups - 1,))],
        compiler_params=pltpu.CompilerParams(vmem_limit_bytes=TAIL_LIMIT),
    )(*results)


def cuts(planes):
    if planes < 3:
        return [(p, 1) for p in range(planes)]
    first = max(1, planes * 2 // 16)
    last = max(1, planes * 6 // 16)
    return [(0, first), (first, planes - first - last), (planes - last, last)]


def staged_local(source, basis_x, basis_y, basis_z, eigen_x, eigen_y, eigen_z):
    rows_n = lax.axis_size("row")
    cols_n = lax.axis_size("col")
    devices = rows_n * cols_n
    me = lax.axis_index("row") * cols_n + lax.axis_index("col")
    ax, by, nz = source.shape
    nx, ny = basis_x.shape[0], basis_y.shape[0]
    planes = nz // devices
    bz = basis_z.reshape(nz, devices, planes)
    ez = lax.dynamic_slice_in_dim(eigen_z, me * planes, planes, 0)
    exy = eigen_x[:, None] + eigen_y[None, :]
    pieces = cuts(planes)

    def columns(piece):
        start, count = piece
        return bz[:, :, start : start + count].reshape(nz, devices * count)

    def exchange(field):
        return lax.all_to_all(field, ("row", "col"), split_axis=0, concat_axis=0, tiled=True)

    def forward(piece):
        field = jnp.einsum("ck,abc->kab", columns(piece), source, precision=FAST)
        return with_layout_constraint(field, Layout(major_to_minor=(0, 1, 2)))

    def middle(piece, field):
        start, count = piece
        field = field.reshape(rows_n, cols_n, count, ax, by)
        field = field.transpose(2, 0, 3, 1, 4).reshape(count, nx, ny)
        field = jnp.einsum("xi,kxy->kiy", basis_x, field, precision=FULL)
        field = jnp.einsum("kiy,yj->kij", field, basis_y, precision=FULL)
        field = field / (exy[None] + ez[start : start + count][:, None, None])
        field = jnp.einsum("kij,yj->kiy", field, basis_y, precision=FULL)
        field = jnp.einsum("xi,kiy->kxy", basis_x, field, precision=FULL)
        field = field.reshape(count, rows_n, ax, cols_n, by).transpose(1, 3, 0, 2, 4)
        return field.reshape(devices * count, ax, by)

    def backward(piece, field, precision):
        return jnp.einsum("ck,kab->abc", columns(piece), field, precision=precision)

    count = len(pieces)
    tie = lax.optimization_barrier
    fields = [forward(pieces[0])]
    arrived = [exchange(fields[0])]
    done = []
    for n in range(1, count):
        field = forward(pieces[n])
        if done:
            arrived[-1], field, done[-1] = tie((arrived[-1], field, done[-1]))
        else:
            arrived[-1], field = tie((arrived[-1], field))
        arrived.append(exchange(field))
        done.append(middle(pieces[n - 1], arrived[n - 1]))
    if done:
        arrived[-1], *done = tie((arrived[-1], *done))
    returned = []
    for n, piece in enumerate(pieces):
        if n == count - 1:
            if count > 2:
                returned[0], arrived[-1] = tie((returned[0], arrived[-1]))
            done.append(middle(piece, arrived[-1]))
        field = done[n]
        if returned:
            returned[-1], field = tie((returned[-1], field))
        returned.append(exchange(field))
    total = backward(pieces[0], returned[0], FULL)
    for piece, field in zip(pieces[1:], returned[1:]):
        total = lax.optimization_barrier(total)
        last = piece is pieces[-1]
        total = total + backward(piece, field, FAST if last else FULL)
    return total


def solution(mesh):
    rows_n, cols_n = mesh.shape["row"], mesh.shape["col"]

    def local(source, basis_x, basis_y, basis_z, *eigen):
        ax, by, nz = source.shape
        square = basis_x.shape == basis_y.shape == basis_z.shape
        planes = nz // (rows_n * cols_n)
        power = not (rows_n & (rows_n - 1) or cols_n & (cols_n - 1))
        room = 4 * (basis_x.shape[0] // LANES) + SUB <= ax
        fits = by == LANES and room and ax % SUB == 0 and planes % SUB == 0
        body = fused_local if square and power and fits else staged_local
        return body(source, basis_x, basis_y, basis_z, *eigen)

    placed = (P("row", "col", None), P(), P(), P(), P(), P(), P())
    return jax.shard_map(
        local, mesh=mesh, in_specs=placed, out_specs=P("row", "col", None), check_vma=False
    )
```

```python
import functools

import jax
import jax.numpy as jnp
from jax import lax
from jax.experimental import pallas as pl
from jax.experimental.layout import Layout, with_layout_constraint
from jax.experimental.pallas import tpu as pltpu
from jax.sharding import PartitionSpec as P

FAST = lax.Precision.HIGH
FULL = lax.Precision.HIGHEST
MESH = pl.DeviceIdType.MESH
LANES = 128
SUB = 8
LIMIT = 45 << 20
TAIL_LIMIT = 20 << 20


def split(value):
    high = value.astype(jnp.bfloat16)
    low = (value - high.astype(jnp.float32)).astype(jnp.bfloat16)
    return high, low


def product(left, right, dims=((1,), (0,))):
    dot = functools.partial(
        lax.dot_general, dimension_numbers=(dims, ((), ())), preferred_element_type=jnp.float32
    )
    (lh, ll), (rh, rl) = left, right
    return dot(lh, rh) + (dot(lh, rl) + dot(ll, rh))


def partners(rows_n, cols_n):
    half = cols_n // 2
    near, far = list(range(half)), list(range(half, cols_n))
    return [(r, c) for r in range(rows_n) for c in far] + [
        (r, c) for r in range(rows_n) for c in reversed(near)
    ]


def fused(
    rows_n, cols_n,
    source, basis_x, basis_y, basis_z, eigen_x, eigen_y, eigen_z,
    out, last, z_high, z_low,
    stage, arrived, x_high, x_low, xt_high, xt_low, y_high, y_low, yt_high, yt_low,
    exy, ex, ey, ez, eigen_sem, load_sem, basis_sem, send1, recv1, send2, recv2, credit,
):
    ax, by, nz = source.shape
    devices = rows_n * cols_n
    planes, _, nx, _ = stage.shape
    chunks, groups = planes // SUB, ax // SUB
    part = devices * SUB
    row, col = lax.axis_index("row"), lax.axis_index("col")
    me = row * cols_n + col
    order = partners(rows_n, cols_n)
    stage_flat = stage.reshape(planes * cols_n * nx, by)
    arrived_flat = arrived.reshape(planes * cols_n * nx, by)
    lines = arrived.reshape(chunks, devices, SUB, ax, by)
    chunk_rows = SUB * cols_n * nx

    side, depth = nx // by, (ax - 4 * (nx // by)) // SUB

    def slot_at(step):
        return pl.ds(4 * side + lax.rem(step, depth) * SUB, SUB)

    def load(step):
        rows = pl.ds(lax.rem(step, groups) * SUB, SUB)
        return pltpu.make_async_copy(source.at[rows], out.at[slot_at(step)], load_sem.at[lax.rem(step, depth)])

    def basis_at(n):
        return pl.ds(n * side, side)

    def basis_copy(ref, n):
        return pltpu.make_async_copy(ref.reshape(side, by, ref.shape[1]), out.at[basis_at(n)], basis_sem.at[n])

    eigen = [(eigen_x, ex.at[0]), (eigen_y, ey.at[0]), (eigen_z, ez)]
    eigen = [pltpu.make_async_copy(a, b, eigen_sem.at[n]) for n, (a, b) in enumerate(eigen)]

    basis_copy(basis_z, 0).start()
    load(jnp.int32(0)).start()
    barrier = pltpu.get_barrier_semaphore()
    for r, c in order:
        if r or c:
            pl.semaphore_signal(barrier, inc=1, device_id=(row ^ r, col ^ c), device_id_type=MESH)

    def choose(h):
        turned = out[basis_at(3)].reshape(nz, nz)
        rows = [turned[d * planes + h * SUB :][:SUB] for d in range(devices)]
        z_high[h], z_low[h] = split(jnp.concatenate(rows, axis=0))

    basis_copy(basis_z, 0).wait()
    out[basis_at(3)] = out[basis_at(0)].reshape(nz, nz).T.reshape(side, by, nz)
    choose(0)

    def exchange(make_src, make_dst, send_sem, recv_sem, offsets=order):
        for r, c in offsets:
            r2, c2 = row ^ r, col ^ c
            if r or c:
                pltpu.make_async_remote_copy(
                    src_ref=make_src(r2, c2), dst_ref=make_dst(), send_sem=send_sem,
                    recv_sem=recv_sem, device_id=(r2, c2), device_id_type=MESH,
                ).start()
            else:
                pltpu.make_async_copy(make_src(r2, c2), make_dst(), recv_sem).start()

    def block(ref, h, r, c, g):
        start = pl.multiple_of(r * ax + g * SUB, SUB)
        return ref.at[pl.ds(h * SUB, SUB), c, pl.ds(start, SUB), :]

    def wait_rows(ref, count, sem):
        view = ref.at[pl.ds(0, count)]
        pltpu.make_async_copy(view, view, sem).wait()

    def forward(step, first=False):
        h, g = step // groups, lax.rem(step, groups)
        load(step).wait()
        for n in range(1, depth if first else 1):
            load(jnp.int32(n)).start()
        lhs = (z_high[h], z_low[h])
        rhs = split(out[slot_at(step)].reshape(SUB * by, nz))
        field = product(lhs, rhs, ((1,), (1,)))
        for n in range(SUB):
            for d in range(devices):
                start = h * chunk_rows + (d % cols_n) * nx + (d // cols_n) * ax + g * SUB + n
                stage_flat[pl.ds(start, SUB, stride=cols_n * nx), :] = field[
                    d * SUB : (d + 1) * SUB, n * by : (n + 1) * by
                ]
        pl.when(step + depth < chunks * groups)(lambda: load(step + depth).start())

    def send_forward(step):
        h, g = step // groups, lax.rem(step, groups)
        exchange(
            lambda r, c: block(stage, h, r, c, g),
            lambda: block(arrived, h, row, col, g),
            send1.at[h], recv1.at[h],
        )

    start = jnp.int32(0)
    forward(start, first=True)
    pl.semaphore_wait(barrier, devices - 1)
    send_forward(start)
    basis_copy(basis_x, 1).start()
    basis_copy(basis_y, 2).start()
    for copy in eigen:
        copy.start()
    for h in range(1, chunks):
        choose(h)

    @pl.loop(1, chunks * groups)
    def _(step):
        forward(step)
        send_forward(step)

    basis_copy(basis_x, 1).wait()
    basis_copy(basis_y, 2).wait()
    for n, natural, turned_refs in ((1, (x_high, x_low), (xt_high, xt_low)), (2, (y_high, y_low), (yt_high, yt_low))):
        value = out[basis_at(n)].reshape(nx, nx)
        natural[0][...], natural[1][...] = split(value)
        turned_refs[0][...], turned_refs[1][...] = split(value.T)
    for copy in eigen:
        copy.wait()
    exy[...] = jnp.broadcast_to(ex[...], exy.shape).T + ey[...]

    def both(pair):
        return pair[0][...], pair[1][...]

    for h in range(chunks):
        wait_rows(arrived_flat, chunk_rows, recv1.at[h])
        wait_rows(stage_flat, (devices - 1) * SUB * ax, send1.at[h])

        @pl.loop(h * SUB, (h + 1) * SUB)
        def _(p):
            field = jnp.concatenate([arrived[p, c] for c in range(cols_n)], axis=1)
            field = product(both((xt_high, xt_low)), split(field))
            field = product(split(field), both((y_high, y_low)))
            field = field / (exy[...] + ez[me * planes + p])
            field = product(split(field), both((yt_high, yt_low)))
            field = product(both((x_high, x_low)), split(field))
            for c in range(cols_n):
                stage[p, c] = field[:, c * by : (c + 1) * by]

        for r, c in order:
            if r or c:
                pl.semaphore_signal(credit.at[h], inc=1, device_id=(row ^ r, col ^ c), device_id_type=MESH)
        pl.semaphore_wait(credit.at[h], devices - 1)

        def line(g):
            return lines.at[h, me, :, pl.ds(pl.multiple_of(g * SUB, SUB), SUB), :]

        def send_back(g, offsets=order, target=line):
            exchange(
                lambda r, c: block(stage, h, r, c, g),
                lambda: target(g),
                send2.at[h], recv2.at[h, g], offsets,
            )

        final = h == chunks - 1

        @pl.loop(0, groups - final)
        def _(g):
            send_back(g)

        if final:
            half = cols_n // 2
            columns = [*range(half, cols_n), *reversed(range(half))]
            send_back(groups - 1, [(r, c) for c in columns for r in range(rows_n)], lambda g: last.at[me])

    for h in range(chunks):

        @pl.loop(0, groups - (h == chunks - 1))
        def _(g):
            wait_rows(arrived_flat, part * SUB, recv2.at[h, g])
            a = g * SUB
            sides = [
                arrived_flat[pl.ds(h * chunk_rows + a + n, part, stride=ax), :].T for n in range(SUB)
            ]
            field = backward(sides, z_high[h], z_low[h])
            if h:
                field = field + out[pl.ds(a, SUB)]
            out[pl.ds(a, SUB)] = field

    h, g = chunks - 1, groups - 1
    pltpu.make_async_copy(last, last, recv2.at[h, g]).wait()
    for h in range(chunks):
        wait_rows(stage_flat, (devices - 1) * SUB * ax, send2.at[h])


def backward(sides, z_high, z_low):
    field = product(split(jnp.concatenate(sides, axis=0)), (z_high, z_low))
    return field.reshape(len(sides), -1, field.shape[1])


def finish(most, last, z_high, z_low, out, tail, sems):
    start = out.shape[0] - SUB
    step = start // (sems.shape[0] - 1)
    copies = [
        pltpu.make_async_copy(most.at[pl.ds(n * step, step)], out.at[pl.ds(n * step, step)], sems.at[n])
        for n in range(sems.shape[0] - 1)
    ]
    copies.append(pltpu.make_async_copy(tail, out.at[pl.ds(start, SUB)], sems.at[sems.shape[0] - 1]))
    for copy in copies[:-1]:
        copy.start()
    part = last.shape[0] * SUB
    rows = last.reshape(part * SUB, last.shape[3])
    sides = [rows[pl.ds(n, part, stride=SUB), :].T for n in range(SUB)]
    field = backward(sides, z_high[z_high.shape[0] - 1], z_low[z_low.shape[0] - 1])
    tail[...] = field + most[pl.ds(start, SUB)]
    copies[-1].start()
    for copy in copies:
        copy.wait()


def fused_local(source, basis_x, basis_y, basis_z, eigen_x, eigen_y, eigen_z):
    rows_n, cols_n = lax.axis_size("row"), lax.axis_size("col")
    devices = rows_n * cols_n
    ax, by, nz = source.shape
    nx, ny = basis_x.shape[0], basis_y.shape[0]
    planes = nz // devices
    chunks, groups = planes // SUB, ax // SUB
    dma, any_space = pltpu.SemaphoreType.DMA, pl.BlockSpec(memory_space=pl.ANY)
    vmem = pl.BlockSpec(memory_space=pltpu.VMEM)
    field = pltpu.VMEM((planes, cols_n, nx, by), jnp.float32)
    zb = pltpu.VMEM((chunks, devices * SUB, nz), jnp.bfloat16)
    xb = pltpu.VMEM((nx, nx), jnp.bfloat16)
    yb = pltpu.VMEM((ny, ny), jnp.bfloat16)
    results = pl.pallas_call(
        functools.partial(fused, rows_n, cols_n),
        out_shape=(
            pltpu.VMEM((ax, by, nz), jnp.float32), pltpu.VMEM((devices, SUB, SUB, by), jnp.float32), zb, zb,
        ),
        in_specs=[any_space] * 7,
        out_specs=(vmem,) * 4,
        scratch_shapes=[
            field, field, xb, xb, xb, xb, yb, yb, yb, yb,
            pltpu.VMEM((nx, ny), jnp.float32), pltpu.VMEM((1, nx), jnp.float32), pltpu.VMEM((1, ny), jnp.float32),
            pltpu.SMEM((nz,), jnp.float32),
            dma((3,)), dma(((ax - 4 * (nx // by)) // SUB,)), dma((3,)), dma((chunks,)), dma((chunks,)), dma((chunks,)), dma((chunks, groups)),
            pltpu.SemaphoreType.REGULAR((chunks,)),
        ],
        compiler_params=pltpu.CompilerParams(
            collective_id=0, has_side_effects=True, vmem_limit_bytes=LIMIT
        ),
    )(source, basis_x, basis_y, basis_z, eigen_x, eigen_y, eigen_z)
    return pl.pallas_call(
        finish,
        out_shape=jax.ShapeDtypeStruct((ax, by, nz), jnp.float32),
        in_specs=[vmem] * 4,
        out_specs=any_space,
        scratch_shapes=[pltpu.VMEM((SUB, by, nz), jnp.float32), dma((2 * groups - 1,))],
        compiler_params=pltpu.CompilerParams(vmem_limit_bytes=TAIL_LIMIT),
    )(*results)


def cuts(planes):
    if planes < 3:
        return [(p, 1) for p in range(planes)]
    first = max(1, planes * 2 // 16)
    last = max(1, planes * 6 // 16)
    return [(0, first), (first, planes - first - last), (planes - last, last)]


def staged_local(source, basis_x, basis_y, basis_z, eigen_x, eigen_y, eigen_z):
    rows_n = lax.axis_size("row")
    cols_n = lax.axis_size("col")
    devices = rows_n * cols_n
    me = lax.axis_index("row") * cols_n + lax.axis_index("col")
    ax, by, nz = source.shape
    nx, ny = basis_x.shape[0], basis_y.shape[0]
    planes = nz // devices
    bz = basis_z.reshape(nz, devices, planes)
    ez = lax.dynamic_slice_in_dim(eigen_z, me * planes, planes, 0)
    exy = eigen_x[:, None] + eigen_y[None, :]
    pieces = cuts(planes)

    def columns(piece):
        start, count = piece
        return bz[:, :, start : start + count].reshape(nz, devices * count)

    def exchange(field):
        return lax.all_to_all(field, ("row", "col"), split_axis=0, concat_axis=0, tiled=True)

    def forward(piece):
        field = jnp.einsum("ck,abc->kab", columns(piece), source, precision=FAST)
        return with_layout_constraint(field, Layout(major_to_minor=(0, 1, 2)))

    def middle(piece, field):
        start, count = piece
        field = field.reshape(rows_n, cols_n, count, ax, by)
        field = field.transpose(2, 0, 3, 1, 4).reshape(count, nx, ny)
        field = jnp.einsum("xi,kxy->kiy", basis_x, field, precision=FULL)
        field = jnp.einsum("kiy,yj->kij", field, basis_y, precision=FULL)
        field = field / (exy[None] + ez[start : start + count][:, None, None])
        field = jnp.einsum("kij,yj->kiy", field, basis_y, precision=FULL)
        field = jnp.einsum("xi,kiy->kxy", basis_x, field, precision=FULL)
        field = field.reshape(count, rows_n, ax, cols_n, by).transpose(1, 3, 0, 2, 4)
        return field.reshape(devices * count, ax, by)

    def backward(piece, field, precision):
        return jnp.einsum("ck,kab->abc", columns(piece), field, precision=precision)

    count = len(pieces)
    tie = lax.optimization_barrier
    fields = [forward(pieces[0])]
    arrived = [exchange(fields[0])]
    done = []
    for n in range(1, count):
        field = forward(pieces[n])
        if done:
            arrived[-1], field, done[-1] = tie((arrived[-1], field, done[-1]))
        else:
            arrived[-1], field = tie((arrived[-1], field))
        arrived.append(exchange(field))
        done.append(middle(pieces[n - 1], arrived[n - 1]))
    if done:
        arrived[-1], *done = tie((arrived[-1], *done))
    returned = []
    for n, piece in enumerate(pieces):
        if n == count - 1:
            if count > 2:
                returned[0], arrived[-1] = tie((returned[0], arrived[-1]))
            done.append(middle(piece, arrived[-1]))
        field = done[n]
        if returned:
            returned[-1], field = tie((returned[-1], field))
        returned.append(exchange(field))
    total = backward(pieces[0], returned[0], FULL)
    for piece, field in zip(pieces[1:], returned[1:]):
        total = lax.optimization_barrier(total)
        last = piece is pieces[-1]
        total = total + backward(piece, field, FAST if last else FULL)
    return total


def solution(mesh):
    rows_n, cols_n = mesh.shape["row"], mesh.shape["col"]

    def local(source, basis_x, basis_y, basis_z, *eigen):
        ax, by, nz = source.shape
        square = basis_x.shape == basis_y.shape == basis_z.shape
        planes = nz // (rows_n * cols_n)
        power = not (rows_n & (rows_n - 1) or cols_n & (cols_n - 1))
        room = 4 * (basis_x.shape[0] // LANES) + SUB <= ax
        fits = by == LANES and room and ax % SUB == 0 and planes % SUB == 0
        body = fused_local if square and power and fits else staged_local
        return body(source, basis_x, basis_y, basis_z, *eigen)

    placed = (P("row", "col", None), P(), P(), P(), P(), P(), P())
    return jax.shard_map(
        local, mesh=mesh, in_specs=placed, out_specs=P("row", "col", None), check_vma=False
    )
```
